32 devices in a mesh: seq: 16 (over z, y, x), rep: 2 (over core).
Axes of the slice: x: 2, y: 2, z: 4, core: 2. Of those that a mesh axis runs over, the one named last changes fastest.
Arguments:
- queries: bfloat16 [4096, 4096], P(('rep', 'seq')), parts along dimension 0, may hold values from -160 to 160
- keys_values: bfloat16 [2, 4096, 1024], P(None, ('rep', 'seq')), parts along dimension 1, may hold values from -6 to 6
- segment_ids: int32 [4096], P(('rep', 'seq')), parts along dimension 0, may hold values from 0 to 31, never falling along the last dimension, each value on 1 to 1024 neighbouring positions
Outputs:
- attended: bfloat16 [4096, 4096], P(('rep', 'seq')), parts along dimension 0
The draws below stay inside these ranges and needn't reach their ends.
There are 2 independent parts, one for each index of `rep`. The reference program is written for one: setup_inputs(seed, part) draws one part's arguments, and reference() takes and returns one part's arrays. A program takes and returns all parts, laid end to end along the dimension named above; each array names one. Nothing has to cross between parts.
Inputs may be any that keep to these rules, and one draw needn't show every extreme that they name: `segment_ids`: ids never fall along the tokens; every document holds 1 to 1024 consecutive tokens, one exactly 1024.
All inputs are finite; a program needn't handle non-finite values.
Results may differ from the reference program's by a relative error of at most 0.004.
Values may be sent and summed in bfloat16 or wider, within the bound.
A program may use at most 192 MiB of HBM per device.

```python
import math
import jax
import jax.numpy as jnp
import numpy as np
from jax import lax

HQ = 32
HK = 8
DH = 128
WINDOW = 2048
DOC_COUNT = 32
TOKENS = 2048
DOC_MOST = 1024


def shared_draw(key):
    shape_keys = (TOKENS, HK * DH)
    key_rows = jnp.clip(jax.random.normal(jax.random.fold_in(key, 101), shape_keys, jnp.float32), -6.0, 6.0)
    value_rows = jnp.clip(jax.random.normal(jax.random.fold_in(key, 102), shape_keys, jnp.float32), -6.0, 6.0)
    query_rows = jnp.clip(jax.random.normal(jax.random.fold_in(key, 103), (TOKENS, HQ * DH), jnp.float32), -6.0, 6.0)
    return (query_rows, jnp.stack([key_rows, value_rows]))


def draw_queries(key, part):
    return shared_draw(key)[0].astype(jnp.bfloat16)


def draw_keys_values(key, part):
    return shared_draw(key)[1].astype(jnp.bfloat16)


def length_profile(amount, total, limit, slope):
    weights = [(1 << 20) // math.isqrt(standing ** slope) + 1 for standing in range(2, amount + 1)]
    spare, given = total - limit - (amount - 1), [1] * (amount - 1)
    while spare > 0:
        free = [i for i in range(amount - 1) if given[i] < limit]
        whole, budget = sum([weights[i] for i in free]), spare
        for i in free:
            addition = min(limit - given[i], max(1, budget * weights[i] // whole), spare)
            given[i] = given[i] + addition
            spare = spare - addition
    return np.array([limit] + given)


def uneven_parts(own_key, number_of, total, limit, skew):
    if number_of == 2:
        one = jax.random.randint(own_key, (), max(1, total - limit), min(limit, total - 1) + 1)
        return jnp.stack([one, total - one])
    tallies = jnp.asarray(length_profile(number_of, total, limit, skew), jnp.int32)
    couples = (number_of - 1) // 2
    donor, receiver = tallies[1:1 + 2 * couples:2], tallies[2:2 + 2 * couples:2]
    room = jnp.minimum(donor - 1, limit - receiver)
    moved = jax.random.randint(jax.random.fold_in(own_key, 1), (couples,), 0, 1 << 20) % (room + 1)
    tallies = tallies.at[1:1 + 2 * couples:2].set(donor - moved).at[2:2 + 2 * couples:2].set(receiver + moved)
    return tallies[jax.random.permutation(jax.random.fold_in(own_key, 2), number_of)]


def setup_inputs(seed: int = 0, part: int = 0) -> dict:
    streams_of = jax.random.split(jax.random.key(seed), 4)
    part_keys = jax.random.split(jax.random.fold_in(streams_of[3], part), 4)
    queries = draw_queries(jax.random.fold_in(jax.random.fold_in(streams_of[3], part), 71), part)
    keys_values = draw_keys_values(jax.random.fold_in(jax.random.fold_in(streams_of[3], part), 71), part)
    segment_ids = jnp.searchsorted(jnp.cumsum(uneven_parts(part_keys[2], DOC_COUNT, TOKENS, DOC_MOST, 2)), jnp.arange(TOKENS), side="right").astype(jnp.int32)
    return dict(queries=queries, keys_values=keys_values, segment_ids=segment_ids)


def reference(queries, keys_values, segment_ids):
    group_size = HQ // HK
    score_scale = DH ** -0.5
    query_rows = min(512, TOKENS)
    key_span = WINDOW + query_rows
    key_table = jnp.pad(keys_values[0], ((WINDOW, 0), (0, 0)))
    value_table = jnp.pad(keys_values[1], ((WINDOW, 0), (0, 0)))
    padded_ids = jnp.pad(segment_ids, (WINDOW, 0), constant_values=-1)

    def one_block(number):
        first_row = (number * query_rows).astype(jnp.int32)
        query_block = lax.dynamic_slice_in_dim(queries, first_row, query_rows, 0)
        query_block = query_block.reshape(query_rows, HK, group_size, DH).astype(jnp.float32)
        key_block = lax.dynamic_slice_in_dim(key_table, first_row, key_span, 0).reshape(key_span, HK, DH).astype(jnp.float32)
        value_block = lax.dynamic_slice_in_dim(value_table, first_row, key_span, 0).reshape(key_span, HK, DH).astype(jnp.float32)
        query_ids = lax.dynamic_slice_in_dim(segment_ids, first_row, query_rows, 0)
        key_ids = lax.dynamic_slice_in_dim(padded_ids, first_row, key_span, 0)
        query_place = jnp.arange(query_rows, dtype=jnp.int32) + WINDOW
        key_place = jnp.arange(key_span, dtype=jnp.int32)
        distance = query_place[:, None] - key_place[None, :]
        allowed = (query_ids[:, None] == key_ids[None, :]) & (distance >= 0) & (distance < WINDOW)
        scores = jnp.einsum("qhgd,khd->hgqk", query_block, key_block) * score_scale
        scores = jnp.where(allowed, scores, -1.0e30)
        top = jnp.max(scores, axis=-1, keepdims=True)
        weights = jnp.where(allowed, jnp.exp(scores - top), 0.0)
        totals = jnp.sum(weights, axis=-1)
        rounded = lax.optimization_barrier(weights.astype(jnp.bfloat16))
        context = jnp.einsum("hgqk,khd->hgqd", rounded.astype(jnp.float32), value_block)
        result = context / totals[..., None]
        return jnp.transpose(result, (2, 0, 1, 3)).reshape(query_rows, HQ * DH).astype(jnp.bfloat16)

    blocks = lax.map(one_block, jnp.arange(TOKENS // query_rows, dtype=jnp.int32))
    return blocks.reshape(TOKENS, HQ * DH)
```

```python
import functools
import math

import jax
import jax.numpy as jnp
from jax import lax
from jax.experimental import pallas as pl
from jax.experimental.pallas import tpu as pltpu
from jax.sharding import PartitionSpec as P

HQ = 32
HK = 8
DH = 128
WINDOW = 2048
GROUP = HQ // HK
SPAN = 4
CHUNKS = 4
PER = HK // CHUNKS
NEG_BIG = -1e30
SCALE2 = DH ** (-0.5) * math.log2(math.e)


def kernel(n, rows, back, q_hbm, kv_hbm, ids_hbm, out_hbm, buf, ids_buf, q_buf, out_buf, bias, run_max, run_sum, run_acc,
           in_sem, out_sem, send_sem, recv_sem):
    last = back // SPAN
    planes = n // SPAN
    me = lax.axis_index("seq")
    plane = me // SPAN
    spot = me % SPAN
    low, high = spot % 2, spot // 2
    spot_x = (1 - low) + 2 * high
    spot_y = low + 2 * (1 - high)
    spot_d = (1 - low) + 2 * (1 - high)
    spots = (spot, spot_x, spot_y, spot_d)
    dev_x = plane * SPAN + spot_x
    dev_y = plane * SPAN + spot_y
    up_ok = plane < planes - 1
    down_ok = plane > 0
    dev_up = jnp.where(up_ok, me + SPAN, me - SPAN)
    dev_down = jnp.where(down_ok, me - SPAN, me + SPAN)
    ids_piece = CHUNKS

    def need(s, to, block):
        gap = SPAN * s + to - block
        return (plane >= s) & (gap >= 1) & (gap <= back)

    def via_x(s, block, c):
        mixed = (block % 2) != (block // 2)
        first = c < CHUNKS // 2 or c == ids_piece
        middle = 0 < s < last
        if first and middle:
            return block >= 0
        if first:
            return jnp.logical_not(mixed)
        if middle:
            return mixed
        return block < 0

    def ref_of(s, r, c):
        if c == ids_piece:
            return ids_buf.at[s, r]
        return buf.at[s, pl.ds(c * PER, PER), :, r]

    def copy(s, r, c, lane, to_s, to_r, device):
        return pltpu.make_async_remote_copy(
            src_ref=ref_of(s, r, c),
            dst_ref=ref_of(to_s, to_r, c),
            send_sem=send_sem.at[s, lane, c],
            recv_sem=recv_sem.at[to_s, to_r, c],
            device_id={"seq": device},
            device_id_type=pl.DeviceIdType.MESH,
        )

    def forwards(s, c):
        out = [
            (need(s, spot_x, spot), copy(s, 0, c, 0, s, 1, dev_x)),
            (need(s, spot_y, spot), copy(s, 0, c, 1, s, 2, dev_y)),
        ]
        if s < last:
            out.insert(0, (up_ok & (plane >= s), copy(s, 0, c, 2, s + 1, 0, dev_up)))
        return out

    def relay_x(s, c):
        return (need(s, spot_y, spot_x) & via_x(s, spot_x, c), copy(s, 1, c, 3, s, 3, dev_y))

    def relay_y(s, c):
        return (need(s, spot_x, spot_y) & jnp.logical_not(via_x(s, spot_y, c)), copy(s, 2, c, 4, s, 3, dev_x))

    def start(pair):
        @pl.when(pair[0])
        def _():
            pair[1].start()

    def wait_in(s, r, c):
        cond = (plane >= s) if r == 0 else need(s, spot, spots[r])

        @pl.when(cond)
        def _():
            copy(s, r, c, 0, s, r, dev_x).wait_recv()

    kv_in = [
        pltpu.make_async_copy(kv_hbm.at[:, :, pl.ds(h * DH, DH)], buf.at[0, h, :, 0], in_sem.at[h]) for h in range(HK)
    ]
    ids_in = pltpu.make_async_copy(ids_hbm, ids_buf.at[0, 0], in_sem.at[HK])
    q_in = pltpu.make_async_copy(q_hbm, q_buf, in_sem.at[HK + 1])
    ids_in.start()
    for one in kv_in:
        one.start()
    q_in.start()

    barrier = pltpu.get_barrier_semaphore()
    for cond, device in ((None, dev_x), (None, dev_y), (up_ok, dev_up), (down_ok, dev_down)):
        def greet(device=device):
            pl.semaphore_signal(barrier, inc=1, device_id={"seq": device}, device_id_type=pl.DeviceIdType.MESH)
        if cond is None:
            greet()
        else:
            pl.when(cond)(greet)
    pl.semaphore_wait(barrier, 2 + up_ok.astype(jnp.int32) + down_ok.astype(jnp.int32))

    pieces = [ids_piece] + list(range(CHUNKS))
    for c in pieces:
        if c == ids_piece:
            ids_in.wait()
        else:
            for h in range(c * PER, (c + 1) * PER):
                kv_in[h].wait()
        for pair in forwards(0, c):
            start(pair)

    for s in range(last + 1):
        for r in range(SPAN):
            if s == 0 and r == 0:
                continue
            absent = (plane < s) if r == 0 else jnp.logical_not(need(s, spot, spots[r]))

            @pl.when(absent)
            def _():
                ids_buf[s, r] = jnp.zeros((1, rows), jnp.int32)

                def clear(h, carry):
                    for k in range(2):
                        buf[s, h, k, r] = jnp.zeros((rows, DH), buf.dtype)
                    return carry

                lax.fori_loop(0, HK, clear, 0)

    q_in.wait()

    def make_bias(s):
        own = jnp.broadcast_to(ids_buf[0, 0].astype(jnp.float32), (rows, rows)).T
        row = lax.broadcasted_iota(jnp.int32, (rows, rows), 0)
        col = lax.broadcasted_iota(jnp.int32, (rows, rows), 1)
        for r in range(SPAN):
            gap = SPAN * s + spot - spots[r]
            limit = jnp.where((plane >= s) & (gap <= back), WINDOW, 0)
            distance = gap * rows + row - col
            other = jnp.broadcast_to(ids_buf[s, r].astype(jnp.float32), (rows, rows))
            allowed = (own == other) & (distance >= 0) & (distance < limit)
            bias[s, :, r * rows:(r + 1) * rows] = jnp.where(allowed, 0.0, NEG_BIG)

    def attend(s, h):
        cols = pl.ds(pl.multiple_of(h * GROUP * DH, GROUP * DH), GROUP * DH)
        wide = q_buf[:, cols]
        q = jnp.concatenate([wide[:, g * DH:(g + 1) * DH] for g in range(GROUP)], axis=0)
        k = buf[s, h, 0].reshape(SPAN * rows, DH)
        v = buf[s, h, 1].reshape(SPAN * rows, DH)
        t = lax.dot_general(q, k, (((1,), (1,)), ((), ())), preferred_element_type=jnp.float32)
        t = (t * SCALE2).reshape(GROUP, rows, SPAN * rows) + bias[s][None]
        t = t.reshape(GROUP * rows, SPAN * rows)
        top = jnp.max(t, axis=1, keepdims=True)
        if s > 0:
            old = run_max[h]
            new = jnp.maximum(old, top)
        else:
            new = jnp.broadcast_to(top, (GROUP * rows, DH))
        p = [jnp.exp2(t[:, r * rows:(r + 1) * rows] - new) for r in range(SPAN)]
        total = (p[0] + p[1]) + (p[2] + p[3])
        w = jnp.concatenate([one.astype(jnp.bfloat16) for one in p], axis=1)
        acc = jnp.dot(w, v, preferred_element_type=jnp.float32)
        if s > 0:
            fix = jnp.exp2(old - new)
            total = total + run_sum[h] * fix
            acc = acc + run_acc[h] * fix
        if s < last:
            run_max[h] = new
            run_sum[h] = total
            run_acc[h] = acc
        else:
            o = (acc / jnp.sum(total, axis=1, keepdims=True)).astype(out_buf.dtype)
            out_buf[:, cols] = jnp.concatenate([o[g * rows:(g + 1) * rows] for g in range(GROUP)], axis=1)

    def out_copy(c):
        cols = pl.ds(c * PER * GROUP * DH, PER * GROUP * DH)
        return pltpu.make_async_copy(out_buf.at[:, cols], out_hbm.at[:, cols], out_sem.at[c])

    def consume(s, c):
        wait_in(s, 3, c)
        if c == ids_piece:
            make_bias(s)
            return

        def body(h, carry):
            attend(s, h)
            return carry

        lax.fori_loop(c * PER, (c + 1) * PER, body, 0)
        if s == last:
            out_copy(c).start()

    late = None
    for s in range(last + 1):
        for c in pieces:
            if s < last:
                wait_in(s + 1, 0, c)
                for pair in forwards(s + 1, c):
                    start(pair)
            wait_in(s, 1, c)
            start(relay_x(s, c))
            wait_in(s, 2, c)
            start(relay_y(s, c))
            if late is not None:
                consume(*late)
            late = (s, c)
    consume(*late)

    for s in range(last + 1):
        for c in pieces:
            for cond, one in forwards(s, c) + [relay_x(s, c), relay_y(s, c)]:
                @pl.when(cond)
                def _():
                    one.wait_send()
    for c in range(CHUNKS):
        out_copy(c).wait()


def solution(mesh):
    n = mesh.shape["seq"]

    def local(queries, keys_values, segment_ids):
        rows = queries.shape[0]
        reach = min(WINDOW, n * rows // 2)
        back = -(-(reach - 1) // rows)
        assert n % SPAN == 0 and back % SPAN == 0
        sets = back // SPAN + 1
        group_rows = GROUP * rows
        return pl.pallas_call(
            functools.partial(kernel, n, rows, back),
            out_shape=jax.ShapeDtypeStruct(queries.shape, queries.dtype),
            in_specs=[pl.BlockSpec(memory_space=pl.ANY)] * 3,
            out_specs=pl.BlockSpec(memory_space=pl.ANY),
            scratch_shapes=[
                pltpu.VMEM((sets, HK, 2, SPAN, rows, DH), jnp.bfloat16),
                pltpu.VMEM((sets, SPAN, 1, rows), jnp.int32),
                pltpu.VMEM((rows, HQ * DH), jnp.bfloat16),
                pltpu.VMEM((rows, HQ * DH), jnp.bfloat16),
                pltpu.VMEM((sets, rows, SPAN * rows), jnp.float32),
                pltpu.VMEM((HK, group_rows, DH), jnp.float32),
                pltpu.VMEM((HK, group_rows, DH), jnp.float32),
                pltpu.VMEM((HK, group_rows, DH), jnp.float32),
                pltpu.SemaphoreType.DMA((HK + 2,)),
                pltpu.SemaphoreType.DMA((CHUNKS,)),
                pltpu.SemaphoreType.DMA((sets, 5, CHUNKS + 1)),
                pltpu.SemaphoreType.DMA((sets, SPAN, CHUNKS + 1)),
            ],
            compiler_params=pltpu.CompilerParams(
                collective_id=0, has_side_effects=True, vmem_limit_bytes=60 * 1024 * 1024
            ),
        )(queries, keys_values, segment_ids.reshape(1, rows))

    return jax.shard_map(
        local,
        mesh=mesh,
        in_specs=(P(("rep", "seq"), None), P(None, ("rep", "seq"), None), P(("rep", "seq"))),
        out_specs=P(("rep", "seq"), None),
        check_vma=False,
    )
```

```python
import functools
import math

import jax
import jax.numpy as jnp
from jax import lax
from jax.experimental import pallas as pl
from jax.experimental.pallas import tpu as pltpu
from jax.sharding import PartitionSpec as P

HQ = 32
HK = 8
DH = 128
WINDOW = 2048
GROUP = HQ // HK
SPAN = 4
CHUNKS = 8
RELAY_LAG, USE_LAG, LAST_LAG, TAIL_LAG = 4, 13, 6, 11
PER = HK // CHUNKS
NEG_BIG = -1e30
SCALE2 = DH ** (-0.5) * math.log2(math.e)


def kernel(n, rows, back, q_hbm, kv_hbm, ids_hbm, out_hbm, buf, ids_buf, q_buf, out_buf, bias, run_max, run_sum, run_acc,
           in_sem, out_sem, send_sem, recv_sem):
    last = back // SPAN
    planes = n // SPAN
    me = lax.axis_index("seq")
    plane = me // SPAN
    spot = me % SPAN
    low, high = spot % 2, spot // 2
    spot_x = (1 - low) + 2 * high
    spot_y = low + 2 * (1 - high)
    spot_d = (1 - low) + 2 * (1 - high)
    spots = (spot, spot_x, spot_y, spot_d)
    dev_x = plane * SPAN + spot_x
    dev_y = plane * SPAN + spot_y
    up_ok = plane < planes - 1
    down_ok = plane > 0
    dev_up = jnp.where(up_ok, me + SPAN, me - SPAN)
    dev_down = jnp.where(down_ok, me - SPAN, me + SPAN)
    ids_piece = CHUNKS

    def need(s, to, block):
        gap = SPAN * s + to - block
        return (plane >= s) & (gap >= 1) & (gap <= back)

    def via_x(s, block, c):
        mixed = (block % 2) != (block // 2)
        first = c < CHUNKS // 2 or c == ids_piece
        middle = 0 < s < last
        if first and middle:
            return block >= 0
        if first:
            return jnp.logical_not(mixed)
        if middle:
            return mixed
        return block < 0

    def ref_of(s, r, c):
        if c == ids_piece:
            return ids_buf.at[s, r]
        return buf.at[s, pl.ds(c * PER, PER), :, r]

    def copy(s, r, c, lane, to_s, to_r, device):
        return pltpu.make_async_remote_copy(
            src_ref=ref_of(s, r, c),
            dst_ref=ref_of(to_s, to_r, c),
            send_sem=send_sem.at[s, lane, c],
            recv_sem=recv_sem.at[to_s, to_r, c],
            device_id={"seq": device},
            device_id_type=pl.DeviceIdType.MESH,
        )

    def forwards(s, c):
        out = [
            (need(s, spot_x, spot), copy(s, 0, c, 0, s, 1, dev_x)),
            (need(s, spot_y, spot), copy(s, 0, c, 1, s, 2, dev_y)),
        ]
        if s < last:
            out.insert(0, (up_ok & (plane >= s), copy(s, 0, c, 2, s + 1, 0, dev_up)))
        return out

    def relay_x(s, c):
        return (need(s, spot_y, spot_x) & via_x(s, spot_x, c), copy(s, 1, c, 3, s, 3, dev_y))

    def relay_y(s, c):
        return (need(s, spot_x, spot_y) & jnp.logical_not(via_x(s, spot_y, c)), copy(s, 2, c, 4, s, 3, dev_x))

    def start(pair):
        @pl.when(pair[0])
        def _():
            pair[1].start()

    def wait_in(s, r, c):
        cond = (plane >= s) if r == 0 else need(s, spot, spots[r])

        @pl.when(cond)
        def _():
            copy(s, r, c, 0, s, r, dev_x).wait_recv()

    kv_in = [
        pltpu.make_async_copy(kv_hbm.at[:, :, pl.ds(h * DH, DH)], buf.at[0, h, :, 0], in_sem.at[h]) for h in range(HK)
    ]
    ids_in = pltpu.make_async_copy(ids_hbm, ids_buf.at[0, 0], in_sem.at[HK])
    q_in = pltpu.make_async_copy(q_hbm, q_buf, in_sem.at[HK + 1])
    ids_in.start()
    for one in kv_in:
        one.start()
    q_in.start()

    barrier = pltpu.get_barrier_semaphore()
    for cond, device in ((None, dev_x), (None, dev_y), (up_ok, dev_up), (down_ok, dev_down)):
        def greet(device=device):
            pl.semaphore_signal(barrier, inc=1, device_id={"seq": device}, device_id_type=pl.DeviceIdType.MESH)
        if cond is None:
            greet()
        else:
            pl.when(cond)(greet)
    pl.semaphore_wait(barrier, 2 + up_ok.astype(jnp.int32) + down_ok.astype(jnp.int32))

    pieces = [ids_piece] + list(range(CHUNKS))
    for c in pieces:
        if c == ids_piece:
            ids_in.wait()
        else:
            for h in range(c * PER, (c + 1) * PER):
                kv_in[h].wait()
        for pair in forwards(0, c):
            start(pair)

    for s in range(last + 1):
        for r in range(SPAN):
            if s == 0 and r == 0:
                continue
            absent = (plane < s) if r == 0 else jnp.logical_not(need(s, spot, spots[r]))

            @pl.when(absent)
            def _():
                ids_buf[s, r] = jnp.zeros((1, rows), jnp.int32)

                def clear(h, carry):
                    for k in range(2):
                        buf[s, h, k, r] = jnp.zeros((rows, DH), buf.dtype)
                    return carry

                lax.fori_loop(0, HK, clear, 0)

    q_in.wait()

    def make_bias(s, begin, end):
        own = jnp.broadcast_to(ids_buf[0, 0].astype(jnp.float32), (rows, rows)).T
        row = lax.broadcasted_iota(jnp.int32, (rows, rows), 0)
        col = lax.broadcasted_iota(jnp.int32, (rows, rows), 1)
        for r in range(begin, end):
            gap = SPAN * s + spot - spots[r]
            limit = jnp.where((plane >= s) & (gap <= back), WINDOW, 0)
            distance = gap * rows + row - col
            other = jnp.broadcast_to(ids_buf[s, r].astype(jnp.float32), (rows, rows))
            allowed = (own == other) & (distance >= 0) & (distance < limit)
            bias[s, :, r * rows:(r + 1) * rows] = jnp.where(allowed, 0.0, NEG_BIG)

    def attend(s, h, begin, end):
        first, final = s == 0, s == last and end == SPAN
        span = (end - begin) * rows
        cols = pl.ds(pl.multiple_of(h * GROUP * DH, GROUP * DH), GROUP * DH)
        wide = q_buf[:, cols]
        q = jnp.concatenate([wide[:, g * DH:(g + 1) * DH] for g in range(GROUP)], axis=0)
        k = buf[s, h, 0, begin:end].reshape(span, DH)
        v = buf[s, h, 1, begin:end].reshape(span, DH)
        t = lax.dot_general(q, k, (((1,), (1,)), ((), ())), preferred_element_type=jnp.float32)
        t = (t * SCALE2).reshape(GROUP, rows, span) + bias[s, :, begin * rows:end * rows][None]
        t = t.reshape(GROUP * rows, span)
        top = jnp.max(t, axis=1, keepdims=True)
        if first:
            new = jnp.broadcast_to(top, (GROUP * rows, DH))
        else:
            old = run_max[h]
            new = jnp.maximum(old, top)
        p = [jnp.exp2(t[:, r * rows:(r + 1) * rows] - new) for r in range(end - begin)]
        total = functools.reduce(lambda x, y: x + y, p)
        w = jnp.concatenate([one.astype(jnp.bfloat16) for one in p], axis=1)
        acc = jnp.dot(w, v, preferred_element_type=jnp.float32)
        if not first:
            fix = jnp.exp2(old - new)
            total = total + run_sum[h] * fix
            acc = acc + run_acc[h] * fix
        if final:
            o = (acc / jnp.sum(total, axis=1, keepdims=True)).astype(out_buf.dtype)
            out_buf[:, cols] = jnp.concatenate([o[g * rows:(g + 1) * rows] for g in range(GROUP)], axis=1)
        else:
            run_max[h] = new
            run_sum[h] = total
            run_acc[h] = acc

    def out_copy(c):
        cols = pl.ds(c * PER * GROUP * DH, PER * GROUP * DH)
        return pltpu.make_async_copy(out_buf.at[:, cols], out_hbm.at[:, cols], out_sem.at[c])

    def consume(s, c, begin, end):
        if end == SPAN:
            wait_in(s, SPAN - 1, c)
        if c == ids_piece:
            make_bias(s, begin, end)
            return

        def body(h, carry):
            attend(s, h, begin, end)
            return carry

        lax.fori_loop(c * PER, (c + 1) * PER, body, 0)
        if s == last and end == SPAN:
            out_copy(c).start()

    def pass_on(s, c):
        wait_in(s, 0, c)
        for pair in forwards(s, c):
            start(pair)

    def relay(s, c):
        wait_in(s, 1, c)
        start(relay_x(s, c))
        wait_in(s, 2, c)
        start(relay_y(s, c))

    steps = []
    for s in range(last + 1):
        for place, c in enumerate(pieces):
            now = s * len(pieces) + place
            if s > 0:
                steps.append((now - len(pieces), 0, functools.partial(pass_on, s, c)))
            steps.append((now + (RELAY_LAG if 0 < s < last else 0), 1, functools.partial(relay, s, c)))
            if s < last:
                steps.append((now + USE_LAG, 2, functools.partial(consume, s, c, 0, SPAN)))
            else:
                steps.append((now + LAST_LAG, 3, functools.partial(consume, s, c, 0, SPAN - 1)))
                steps.append((now + TAIL_LAG, 4, functools.partial(consume, s, c, SPAN - 1, SPAN)))
    for _, _, step in sorted(steps, key=lambda one: one[:2]):
        step()

    for s in range(last + 1):
        for c in pieces:
            for cond, one in forwards(s, c) + [relay_x(s, c), relay_y(s, c)]:
                @pl.when(cond)
                def _():
                    one.wait_send()
    for c in range(CHUNKS):
        out_copy(c).wait()


def solution(mesh):
    n = mesh.shape["seq"]

    def local(queries, keys_values, segment_ids):
        rows = queries.shape[0]
        reach = min(WINDOW, n * rows // 2)
        back = -(-(reach - 1) // rows)
        assert n % SPAN == 0 and back % SPAN == 0
        sets = back // SPAN + 1
        group_rows = GROUP * rows
        return pl.pallas_call(
            functools.partial(kernel, n, rows, back),
            out_shape=jax.ShapeDtypeStruct(queries.shape, queries.dtype),
            in_specs=[pl.BlockSpec(memory_space=pl.ANY)] * 3,
            out_specs=pl.BlockSpec(memory_space=pl.ANY),
            scratch_shapes=[
                pltpu.VMEM((sets, HK, 2, SPAN, rows, DH), jnp.bfloat16),
                pltpu.VMEM((sets, SPAN, 1, rows), jnp.int32),
                pltpu.VMEM((rows, HQ * DH), jnp.bfloat16),
                pltpu.VMEM((rows, HQ * DH), jnp.bfloat16),
                pltpu.VMEM((sets, rows, SPAN * rows), jnp.float32),
                pltpu.VMEM((HK, group_rows, DH), jnp.float32),
                pltpu.VMEM((HK, group_rows, DH), jnp.float32),
                pltpu.VMEM((HK, group_rows, DH), jnp.float32),
                pltpu.SemaphoreType.DMA((HK + 2,)),
                pltpu.SemaphoreType.DMA((CHUNKS,)),
                pltpu.SemaphoreType.DMA((sets, 5, CHUNKS + 1)),
                pltpu.SemaphoreType.DMA((sets, SPAN, CHUNKS + 1)),
            ],
            compiler_params=pltpu.CompilerParams(
                collective_id=0, has_side_effects=True, vmem_limit_bytes=60 * 1024 * 1024
            ),
        )(queries, keys_values, segment_ids.reshape(1, rows))

    return jax.shard_map(
        local,
        mesh=mesh,
        in_specs=(P(("rep", "seq"), None), P(None, ("rep", "seq"), None), P(("rep", "seq"))),
        out_specs=P(("rep", "seq"), None),
        check_vma=False,
    )
```
